32 devices in a mesh: dp: 1 (over z), ey: 4 (over y), ex: 4 (over x), ec: 2 (over core).
Axes of the slice: x: 4, y: 4, z: 1, core: 2. Of those that a mesh axis runs over, the one named last changes fastest.
The devices are a block of a 4x4x8 slice.
Arguments:
- tokens: bfloat16 [16384, 512], P(('dp', 'ey', 'ex', 'ec'))
- route_idx: int32 [16384, 6], P(('dp', 'ey', 'ex', 'ec'))
- gate_vals: float32 [16384, 6], P(('dp', 'ey', 'ex', 'ec'))
- w_gate: bfloat16 [64, 512, 384], P(('ey', 'ex', 'ec'))
- w_up: bfloat16 [64, 512, 384], P(('ey', 'ex', 'ec'))
- w_down: bfloat16 [64, 384, 512], P(('ey', 'ex', 'ec'))
- ws_gate: bfloat16 [512, 768], replicated
- ws_up: bfloat16 [512, 768], replicated
- ws_down: bfloat16 [768, 512], replicated
- grad_out: bfloat16 [16384, 512], P(('dp', 'ey', 'ex', 'ec'))
Outputs:
- output 1: bfloat16 [16384, 512], P(('dp', 'ey', 'ex', 'ec'))
- output 2: bfloat16 [16384, 512], P(('dp', 'ey', 'ex', 'ec'))
- output 3: float32 [16384, 6], P(('dp', 'ey', 'ex', 'ec'))
- output 4: float32 [64, 512, 384], P(('dp', 'ey', 'ex', 'ec'))
- output 5: float32 [64, 512, 384], P(('dp', 'ey', 'ex', 'ec'))
- output 6: float32 [64, 384, 512], P(('dp', 'ey', 'ex', 'ec'))
- output 7: float32 [32, 512, 768], P(('dp', 'ey', 'ex', 'ec'))
- output 8: float32 [32, 512, 768], P(('dp', 'ey', 'ex', 'ec'))
- output 9: float32 [32, 768, 512], P(('dp', 'ey', 'ex', 'ec'))
All inputs are finite; a program needn't handle non-finite values.
Results may differ from the reference program's by a relative error of at most 0.0103869.
Values are sent between devices in bfloat16 or wider.
A program may use at most 768 MiB of HBM per device.

```python
import jax
import jax.numpy as jnp
from jax import lax

D_MODEL = 512
D_EXPERT = 384
D_SHARED = 768
EXPERTS = 64
TOP_K = 6
TOK_DEV = 512
N_DEV = 32
N_CHIPS = 16

TOKENS = N_DEV * TOK_DEV
HOT_EXP = EXPERTS // N_CHIPS
COLD_EXP = EXPERTS - HOT_EXP
SLOT_CAP = max((TOK_DEV + HOT_EXP - 1) // HOT_EXP, ((TOP_K - 1) * TOK_DEV + COLD_EXP - 1) // COLD_EXP)
ROWS_EXP = N_DEV * SLOT_CAP


def draw_routes(route_key):
    hot_key, dev_root = jax.random.split(route_key)
    hot_start = jax.random.randint(hot_key, (), 0, N_CHIPS) * HOT_EXP

    def one_device(dev_key):
        k_tok, k_hot, k_cold, k_roll = jax.random.split(dev_key, 4)
        tok_pos = jax.random.permutation(k_tok, TOK_DEV)
        hot_perm = jax.random.permutation(k_hot, HOT_EXP)
        cold_perm = jax.random.permutation(k_cold, COLD_EXP)
        hot_ids = hot_start + hot_perm[tok_pos % HOT_EXP]
        cold_pos = tok_pos[:, None] * (TOP_K - 1) + jnp.arange(TOP_K - 1)[None, :]
        cold_ids = (hot_start + HOT_EXP + cold_perm[cold_pos % COLD_EXP]) % EXPERTS
        slot_ids = jnp.concatenate([hot_ids[:, None], cold_ids], axis=1)
        roll_shift = jax.random.randint(k_roll, (TOK_DEV, 1), 0, TOP_K)
        roll_idx = (jnp.arange(TOP_K)[None, :] + roll_shift) % TOP_K
        return jnp.take_along_axis(slot_ids, roll_idx, axis=1)

    routes = jax.vmap(one_device)(jax.random.split(dev_root, N_DEV))
    return routes.reshape(TOKENS, TOP_K).astype(jnp.int32)


def setup_inputs(seed: int = 0, part: int = 0) -> dict:
    part_key = jax.random.fold_in(jax.random.key(seed), part)
    k_tok, k_route, k_gate, k_grad = jax.random.split(part_key, 4)
    w_keys = jax.random.split(jax.random.key(seed + 1), 6)
    model_scale = D_MODEL ** -0.5
    expert_scale = D_EXPERT ** -0.5
    shared_scale = D_SHARED ** -0.5
    tokens = jax.random.normal(k_tok, (TOKENS, D_MODEL), jnp.float32)
    gate_vals = jax.random.uniform(k_gate, (TOKENS, TOP_K), jnp.float32, 0.15, 0.45)
    grad_out = jax.random.normal(k_grad, (TOKENS, D_MODEL), jnp.float32)
    w_gate = jax.random.normal(w_keys[0], (EXPERTS, D_MODEL, D_EXPERT), jnp.float32) * model_scale
    w_up = jax.random.normal(w_keys[1], (EXPERTS, D_MODEL, D_EXPERT), jnp.float32) * model_scale
    w_down = jax.random.normal(w_keys[2], (EXPERTS, D_EXPERT, D_MODEL), jnp.float32) * expert_scale
    ws_gate = jax.random.normal(w_keys[3], (D_MODEL, D_SHARED), jnp.float32) * model_scale
    ws_up = jax.random.normal(w_keys[4], (D_MODEL, D_SHARED), jnp.float32) * model_scale
    ws_down = jax.random.normal(w_keys[5], (D_SHARED, D_MODEL), jnp.float32) * shared_scale
    return {
        "tokens": tokens.astype(jnp.bfloat16),
        "route_idx": draw_routes(k_route),
        "gate_vals": gate_vals,
        "w_gate": w_gate.astype(jnp.bfloat16),
        "w_up": w_up.astype(jnp.bfloat16),
        "w_down": w_down.astype(jnp.bfloat16),
        "ws_gate": ws_gate.astype(jnp.bfloat16),
        "ws_up": ws_up.astype(jnp.bfloat16),
        "ws_down": ws_down.astype(jnp.bfloat16),
        "grad_out": grad_out.astype(jnp.bfloat16),
    }


def swiglu_pass(x_rows, cot_rows, wt_gate, wt_up, wt_down):
    pre_gate = jnp.dot(x_rows, wt_gate, preferred_element_type=jnp.float32).astype(jnp.bfloat16)
    pre_up = jnp.dot(x_rows, wt_up, preferred_element_type=jnp.float32).astype(jnp.bfloat16)
    gate_f32 = pre_gate.astype(jnp.float32)
    up_f32 = pre_up.astype(jnp.float32)
    hidden = (jax.nn.silu(gate_f32) * up_f32).astype(jnp.bfloat16)
    out_rows = jnp.dot(hidden, wt_down, preferred_element_type=jnp.float32).astype(jnp.bfloat16)
    d_hidden = jnp.dot(cot_rows, wt_down.T, preferred_element_type=jnp.float32).astype(jnp.bfloat16)
    dw_down = jnp.dot(hidden.T, cot_rows, preferred_element_type=jnp.float32)
    d_act32 = d_hidden.astype(jnp.float32)
    gate_sig = jax.nn.sigmoid(gate_f32)
    d_gate = (d_act32 * up_f32 * gate_sig * (1.0 + gate_f32 * (1.0 - gate_sig))).astype(jnp.bfloat16)
    d_up = (d_act32 * jax.nn.silu(gate_f32)).astype(jnp.bfloat16)
    dw_gate = jnp.dot(x_rows.T, d_gate, preferred_element_type=jnp.float32)
    dw_up = jnp.dot(x_rows.T, d_up, preferred_element_type=jnp.float32)
    dx_rows = (jnp.dot(d_gate, wt_gate.T, preferred_element_type=jnp.float32)
               + jnp.dot(d_up, wt_up.T, preferred_element_type=jnp.float32)).astype(jnp.bfloat16)
    return out_rows, dx_rows, dw_gate, dw_up, dw_down


def reference(tokens, route_idx, gate_vals, w_gate, w_up, w_down, ws_gate, ws_up, ws_down, grad_out):
    num_slots = TOKENS * TOP_K
    flat_ids = route_idx.reshape(-1)
    slot_order = jnp.argsort(flat_ids, stable=True).astype(jnp.int32)
    counts = jnp.zeros((EXPERTS,), jnp.int32).at[flat_ids].add(1)
    starts = jnp.cumsum(counts) - counts
    sorted_ids = flat_ids[slot_order]
    dest_row = sorted_ids * ROWS_EXP + jnp.arange(num_slots, dtype=jnp.int32) - starts[sorted_ids]
    row_slot = jnp.full((EXPERTS * ROWS_EXP,), num_slots, jnp.int32).at[dest_row].set(slot_order)
    slot_row = jnp.zeros((num_slots,), jnp.int32).at[slot_order].set(dest_row)
    tok_ext = jnp.concatenate([tokens, jnp.zeros((1, D_MODEL), tokens.dtype)])
    grad_ext = jnp.concatenate([grad_out, jnp.zeros((1, D_MODEL), grad_out.dtype)])
    gate_ext = jnp.concatenate([gate_vals.reshape(-1), jnp.zeros((1,), jnp.float32)])

    def expert_pass(operands):
        slot_ids, wt_gate, wt_up, wt_down = operands
        tok_ids = slot_ids // TOP_K
        x_rows = tok_ext[tok_ids]
        cot_rows = (gate_ext[slot_ids][:, None] * grad_ext[tok_ids].astype(jnp.float32)).astype(jnp.bfloat16)
        return swiglu_pass(x_rows, cot_rows, wt_gate, wt_up, wt_down)

    out_rows, dx_rows, dw_gate, dw_up, dw_down = lax.map(
        expert_pass, (row_slot.reshape(EXPERTS, ROWS_EXP), w_gate, w_up, w_down))
    out_flat = out_rows.reshape(EXPERTS * ROWS_EXP, D_MODEL)
    dx_flat = dx_rows.reshape(EXPERTS * ROWS_EXP, D_MODEL)

    def device_pass(operands):
        x_blk, gate_blk, grad_blk, row_blk = operands
        out_slots = out_flat[row_blk].astype(jnp.float32)
        dx_slots = dx_flat[row_blk].astype(jnp.float32)
        s_out, s_dx, dsw_gate, dsw_up, dsw_down = swiglu_pass(x_blk, grad_blk, ws_gate, ws_up, ws_down)
        y_blk = (jnp.sum(gate_blk[:, :, None] * out_slots, axis=1) + s_out.astype(jnp.float32)).astype(jnp.bfloat16)
        dg_blk = jnp.sum(grad_blk.astype(jnp.float32)[:, None, :] * out_slots, axis=2)
        dx_blk = (jnp.sum(dx_slots, axis=1) + s_dx.astype(jnp.float32)).astype(jnp.bfloat16)
        return y_blk, dx_blk, dg_blk, dsw_gate, dsw_up, dsw_down

    y_blocks, dx_blocks, dg_blocks, dws_gate, dws_up, dws_down = lax.map(device_pass, (
        tokens.reshape(N_DEV, TOK_DEV, D_MODEL),
        gate_vals.reshape(N_DEV, TOK_DEV, TOP_K),
        grad_out.reshape(N_DEV, TOK_DEV, D_MODEL),
        slot_row.reshape(N_DEV, TOK_DEV, TOP_K)))
    return (y_blocks.reshape(TOKENS, D_MODEL), dx_blocks.reshape(TOKENS, D_MODEL),
            dg_blocks.reshape(TOKENS, TOP_K), dw_gate, dw_up, dw_down, dws_gate, dws_up, dws_down)
```

```python
import functools

import jax
import jax.numpy as jnp
from jax import lax
from jax.experimental import pallas as pl
from jax.experimental.pallas import tpu as pltpu
from jax.sharding import PartitionSpec as P

EP_AXES = ("ey", "ex", "ec")
ALL_AXES = ("dp", "ey", "ex", "ec")
F32 = jnp.float32
BF16 = jnp.bfloat16
MESH_ID = pl.DeviceIdType.MESH
VMEM_LIMIT = 60 * 1024 * 1024
GROUP = 8


def dot_nn(a, b):
    return lax.dot_general(a, b, (((1,), (0,)), ((), ())), preferred_element_type=F32)


def dot_nt(a, b):
    return lax.dot_general(a, b, (((1,), (1,)), ((), ())), preferred_element_type=F32)


def dot_tn(a, b):
    return lax.dot_general(a, b, (((0,), (0,)), ((), ())), preferred_element_type=F32)


def cparams(**kw):
    return pltpu.CompilerParams(vmem_limit_bytes=VMEM_LIMIT, **kw)


def whole(shape):
    return pl.BlockSpec(shape, lambda *_: (0,) * len(shape))


def swiglu_rows(x, c, w_gate, w_up, w_down):
    u = dot_nn(x, w_gate).astype(BF16).astype(F32)
    v = dot_nn(x, w_up).astype(BF16).astype(F32)
    sig = jax.nn.sigmoid(u)
    silu = u * sig
    a = (silu * v).astype(BF16)
    o = dot_nn(a, w_down).astype(BF16)
    da = dot_nt(c, w_down).astype(BF16).astype(F32)
    du = (da * v * sig * (1.0 + u * (1.0 - sig))).astype(BF16)
    dv = (da * silu).astype(BF16)
    dx = (dot_nt(du, w_gate) + dot_nt(dv, w_up)).astype(BF16)
    return o, dx, a, du, dv


def routing_tables(route_ref, gate_ref, num_exp, hot_exp, local_hot, cap):
    top_k, tok = route_ref.shape
    route = route_ref[...]
    gate = gate_ref[...]
    exp_id = lax.broadcasted_iota(jnp.int32, (num_exp, tok), 0)
    member = jnp.zeros((num_exp, tok), F32)
    gates = jnp.zeros((num_exp, tok), F32)
    for j in range(top_k):
        hit = exp_id == route[j:j + 1, :]
        member = jnp.where(hit, 1.0, member)
        gates = jnp.where(hit, gate[j:j + 1, :], gates)
    before = (lax.broadcasted_iota(jnp.int32, (tok, tok), 0)
              < lax.broadcasted_iota(jnp.int32, (tok, tok), 1)).astype(F32).astype(BF16)
    rank = dot_nn(member.astype(BF16), before)
    counts = jnp.sum(member, axis=1, keepdims=True)
    if not local_hot:
        return jnp.where(member > 0.0, rank, -1.0), gates, None, None, None
    n_sets = num_exp // hot_exp
    set_of = lax.broadcasted_iota(jnp.int32, (n_sets, num_exp), 1) // hot_exp
    in_set = (set_of == lax.broadcasted_iota(jnp.int32, (n_sets, num_exp), 0)).astype(F32).astype(BF16)
    per_set = dot_nn(in_set, member.astype(BF16))
    full = jnp.min(jnp.where(per_set == 1.0, 1.0, 0.0), axis=1, keepdims=True)
    set_id = lax.broadcasted_iota(jnp.int32, (n_sets, 1), 0).astype(F32)
    hot = jnp.min(jnp.where(full > 0.0, set_id, float(n_sets)), axis=0, keepdims=True)
    n_full = jnp.sum(full, axis=0, keepdims=True)
    exp_col = lax.broadcasted_iota(jnp.int32, (num_exp, 1), 0).astype(F32)
    first = hot * float(hot_exp)
    is_hot = jnp.logical_and(exp_col >= first, exp_col < first + float(hot_exp))
    key = jnp.where(member > 0.0, rank, -1.0)
    hot_keys, hot_gates = [], []
    for h in range(hot_exp):
        pick = exp_col == first + float(h)
        hot_keys.append(jnp.sum(jnp.where(pick, key + 1.0, 0.0), axis=0, keepdims=True) - 1.0)
        hot_gates.append(jnp.sum(jnp.where(pick, gates, 0.0), axis=0, keepdims=True))
    key = jnp.where(is_hot, -1.0, key)
    most = jnp.max(jnp.where(is_hot, 0.0, counts), axis=0, keepdims=True)
    bad = jnp.where(jnp.logical_or(most > float(cap), n_full != 1.0), 1.0, 0.0)
    return key, gates, jnp.concatenate(hot_keys, axis=0), jnp.concatenate(hot_gates, axis=0), (hot, bad)


def pick_mask(key_rows, cap):
    tok = key_rows.shape[1]
    rank = lax.broadcasted_iota(jnp.int32, (cap, tok), 0).astype(F32)
    return [key_rows[e:e + 1, :] == rank for e in range(key_rows.shape[0])]


def as_bf16(mask):
    return jnp.where(mask, 1.0, 0.0).astype(BF16)


def gather_x_kernel(route_ref, gate_ref, x_ref, send_ref, key_ref, gates_ref, hkey_ref, hgate_ref, meta_ref,
                    *, num_exp, hot_exp, local_hot, cap):
    i = pl.program_id(0)

    @pl.when(i == 0)
    def _():
        key, gates, hkey, hgate, meta = routing_tables(route_ref, gate_ref, num_exp, hot_exp, local_hot, cap)
        key_ref[...] = key
        gates_ref[...] = gates
        if local_hot:
            hkey_ref[...] = hkey
            hgate_ref[...] = hgate
            lane = lax.broadcasted_iota(jnp.int32, (8, 128), 1)
            meta_ref[...] = jnp.where(lane == 0, meta[0], jnp.where(lane == 1, meta[1], 0.0))
        else:
            hkey_ref[...] = jnp.zeros_like(hkey_ref)
            hgate_ref[...] = jnp.zeros_like(hgate_ref)
            meta_ref[...] = jnp.zeros_like(meta_ref)

    keys = key_ref[pl.ds(pl.multiple_of(i * GROUP, GROUP), GROUP), :]
    x = x_ref[...]
    sel = jnp.concatenate([as_bf16(m) for m in pick_mask(keys, cap)], axis=0)
    send_ref[...] = dot_nn(sel, x).astype(BF16).reshape(send_ref.shape)


def gather_x(route_t, gate_t, tokens, num_exp, hot_exp, local_hot, cap):
    tok, d = tokens.shape
    top_k = route_t.shape[0]
    return pl.pallas_call(
        functools.partial(gather_x_kernel, num_exp=num_exp, hot_exp=hot_exp, local_hot=local_hot, cap=cap),
        grid=(num_exp // GROUP,),
        in_specs=[whole((top_k, tok)), whole((top_k, tok)), whole((tok, d))],
        out_specs=[pl.BlockSpec((GROUP, cap, d), lambda i: (i, 0, 0)), whole((num_exp, tok)), whole((num_exp, tok)),
                   whole((hot_exp, tok)), whole((hot_exp, tok)), whole((8, 128))],
        out_shape=[jax.ShapeDtypeStruct((num_exp, cap, d), BF16), jax.ShapeDtypeStruct((num_exp, tok), F32),
                   jax.ShapeDtypeStruct((num_exp, tok), F32), jax.ShapeDtypeStruct((hot_exp, tok), F32),
                   jax.ShapeDtypeStruct((hot_exp, tok), F32), jax.ShapeDtypeStruct((8, 128), F32)],
        cost_estimate=pl.CostEstimate(flops=2 * num_exp * cap * tok * d, bytes_accessed=2 * num_exp * cap * d,
                                      transcendentals=0),
        compiler_params=cparams(), name="gather_x",
    )(route_t, gate_t, tokens)


def cot_rows(masks, gate_rows, g):
    sel = jnp.concatenate([as_bf16(m) for m in masks], axis=0)
    gate_col = jnp.concatenate(
        [jnp.sum(jnp.where(m, gate_rows[e:e + 1, :], 0.0), axis=1, keepdims=True) for e, m in enumerate(masks)], axis=0)
    return sel, (gate_col * dot_nn(sel, g)).astype(BF16)


def gather_cot_kernel(key_ref, gates_ref, g_ref, send_ref, *, cap):
    masks = pick_mask(key_ref[...], cap)
    send_ref[...] = cot_rows(masks, gates_ref[...], g_ref[...])[1].reshape(send_ref.shape)


def gather_cot(key, gates, grad_out, cap):
    num_exp, tok = key.shape
    d = grad_out.shape[1]
    return pl.pallas_call(
        functools.partial(gather_cot_kernel, cap=cap),
        grid=(num_exp // GROUP,),
        in_specs=[pl.BlockSpec((GROUP, tok), lambda i: (i, 0)), pl.BlockSpec((GROUP, tok), lambda i: (i, 0)),
                  whole((tok, d))],
        out_specs=pl.BlockSpec((GROUP, cap, d), lambda i: (i, 0, 0)),
        out_shape=jax.ShapeDtypeStruct((num_exp, cap, d), BF16),
        cost_estimate=pl.CostEstimate(flops=2 * num_exp * cap * tok * d, bytes_accessed=2 * num_exp * cap * d,
                                      transcendentals=0),
        compiler_params=cparams(), name="gather_cot",
    )(key, gates, grad_out)


def hot_kernel(hkey_ref, hgate_ref, x_ref, g_ref, wg_ref, wu_ref, wd_ref, o_ref, dx_ref, dwg_ref, dwu_ref, dwd_ref,
               *, cap):
    hot_exp = hkey_ref.shape[0]
    for h in range(hot_exp):
        masks = pick_mask(hkey_ref[h:h + 1, :], cap)
        sel, c = cot_rows(masks, hgate_ref[h:h + 1, :], g_ref[...])
        x = dot_nn(sel, x_ref[...]).astype(BF16)
        o, dx, a, du, dv = swiglu_rows(x, c, wg_ref[h], wu_ref[h], wd_ref[h])
        o_ref[h] = o
        dx_ref[h] = dx
        dwd_ref[h] = dot_tn(a, c)
        dwg_ref[h] = dot_tn(x, du)
        dwu_ref[h] = dot_tn(x, dv)


def hot_expert(hkey, hgate, tokens, grad_out, wg, wu, wd, cap):
    hot_exp = hkey.shape[0]
    d, f = wg.shape[1:]
    return pl.pallas_call(
        functools.partial(hot_kernel, cap=cap),
        out_shape=[jax.ShapeDtypeStruct((hot_exp, cap, d), BF16), jax.ShapeDtypeStruct((hot_exp, cap, d), BF16),
                   jax.ShapeDtypeStruct((hot_exp, d, f), F32), jax.ShapeDtypeStruct((hot_exp, d, f), F32),
                   jax.ShapeDtypeStruct((hot_exp, f, d), F32)],
        cost_estimate=pl.CostEstimate(flops=18 * hot_exp * cap * d * f, bytes_accessed=20 * hot_exp * d * f,
                                      transcendentals=0),
        compiler_params=cparams(), name="hot_expert",
    )(hkey, hgate, tokens, grad_out, wg, wu, wd)


def ffn_kernel(x_ref, c_ref, wg_ref, wu_ref, wd_ref, o_ref, dx_ref, dwg_ref, dwu_ref, dwd_ref):
    rows = x_ref.shape[0] * x_ref.shape[2]
    d = x_ref.shape[3]
    x = x_ref[...].reshape(rows, d)
    c = c_ref[...].reshape(rows, d)
    o, dx, a, du, dv = swiglu_rows(x, c, wg_ref[0], wu_ref[0], wd_ref[0])
    o_ref[...] = o.reshape(o_ref.shape)
    dx_ref[...] = dx.reshape(dx_ref.shape)
    first = pl.program_id(1) == 0

    @pl.when(first)
    def _():
        dwd_ref[0] = dot_tn(a, c)
        dwg_ref[0] = dot_tn(x, du)
        dwu_ref[0] = dot_tn(x, dv)

    @pl.when(jnp.logical_not(first))
    def _():
        dwd_ref[0] += dot_tn(a, c)
        dwg_ref[0] += dot_tn(x, du)
        dwu_ref[0] += dot_tn(x, dv)


def ffn(x_rows, c_rows, wg, wu, wd, src_tile):
    n_src, exp_dev, cap, d = x_rows.shape
    f = wg.shape[2]
    row_spec = pl.BlockSpec((src_tile, 1, cap, d), lambda e, s: (s, e, 0, 0))
    up_spec = pl.BlockSpec((1, d, f), lambda e, s: (e, 0, 0))
    down_spec = pl.BlockSpec((1, f, d), lambda e, s: (e, 0, 0))
    rows = n_src * exp_dev * cap
    return pl.pallas_call(
        ffn_kernel, grid=(exp_dev, n_src // src_tile),
        in_specs=[row_spec, row_spec, up_spec, up_spec, down_spec],
        out_specs=[row_spec, row_spec, up_spec, up_spec, down_spec],
        out_shape=[jax.ShapeDtypeStruct(x_rows.shape, BF16), jax.ShapeDtypeStruct(x_rows.shape, BF16),
                   jax.ShapeDtypeStruct(wg.shape, F32), jax.ShapeDtypeStruct(wu.shape, F32),
                   jax.ShapeDtypeStruct(wd.shape, F32)],
        cost_estimate=pl.CostEstimate(flops=18 * rows * d * f, bytes_accessed=8 * rows * d, transcendentals=0),
        compiler_params=cparams(), name="cold_experts",
    )(x_rows, c_rows, wg, wu, wd)


def split3(g):
    hi = g.astype(BF16)
    rest = g - hi.astype(F32)
    mid = rest.astype(BF16)
    lo = (rest - mid.astype(F32)).astype(BF16)
    return hi.astype(F32), mid.astype(F32), lo.astype(F32)


def combine_rows(key_rows, gate_rows, o, dx, g, cap):
    masks = pick_mask(key_rows, cap)
    sel = jnp.concatenate([as_bf16(m) for m in masks], axis=0)
    y = None
    for part in split3(gate_rows):
        wt = jnp.concatenate([jnp.where(m, part[e:e + 1, :], 0.0).astype(BF16) for e, m in enumerate(masks)], axis=0)
        term = dot_tn(wt, o)
        y = term if y is None else y + term
    dxs = dot_tn(sel, dx)
    inner = dot_nt(o, g)
    dg = [jnp.sum(jnp.where(m, inner[e * cap:(e + 1) * cap, :], 0.0), axis=0, keepdims=True)
          for e, m in enumerate(masks)]
    return y, dxs, jnp.concatenate(dg, axis=0)


def combine_kernel(*refs, cap, hot_cap, hot_exp):
    if hot_cap:
        (route_ref, g_ref, s_ref, sdx_ref, key_ref, gates_ref, o_ref, dx_ref, hkey_ref, hgate_ref, ho_ref, hdx_ref,
         y_ref, dxo_ref, dg_ref, yacc, dxacc, dgacc) = refs
    else:
        (route_ref, g_ref, s_ref, sdx_ref, key_ref, gates_ref, o_ref, dx_ref,
         y_ref, dxo_ref, dg_ref, yacc, dxacc, dgacc) = refs
    i = pl.program_id(0)
    g = g_ref[...]
    d = g.shape[1]

    @pl.when(i == 0)
    def _():
        yacc[...] = s_ref[...].astype(F32)
        dxacc[...] = sdx_ref[...].astype(F32)
        dgacc[...] = jnp.zeros_like(dgacc)
        if hot_cap:
            y, dxs, dg = combine_rows(hkey_ref[...], hgate_ref[...], ho_ref[...].reshape(hot_exp * hot_cap, d),
                                      hdx_ref[...].reshape(hot_exp * hot_cap, d), g, hot_cap)
            yacc[...] += y
            dxacc[...] += dxs
            mine = hkey_ref[...] >= 0.0
            dgh = jnp.sum(jnp.where(mine, dg, 0.0), axis=0, keepdims=True)
            dgacc[dgacc.shape[0] - 1:, :] = dgh

    y, dxs, dg = combine_rows(key_ref[...], gates_ref[...], o_ref[...].reshape(GROUP * cap, d),
                              dx_ref[...].reshape(GROUP * cap, d), g, cap)
    yacc[...] += y
    dxacc[...] += dxs
    route = route_ref[...]
    top_k = route.shape[0]
    held = key_ref[...] >= 0.0
    for j in range(top_k):
        exp_id = lax.broadcasted_iota(jnp.int32, dg.shape, 0) + i * GROUP
        hit = jnp.logical_and(exp_id == route[j:j + 1, :], held)
        dgacc[j:j + 1, :] += jnp.sum(jnp.where(hit, dg, 0.0), axis=0, keepdims=True)
        if hot_cap:
            seen = jnp.sum(jnp.where(hit, 1.0, 0.0), axis=0, keepdims=True)
            dg_ref[j:j + 1, :] = jnp.where(i == 0, seen, dg_ref[j:j + 1, :] + seen)

    @pl.when(i == pl.num_programs(0) - 1)
    def _():
        y_ref[...] = yacc[...].astype(BF16)
        dxo_ref[...] = dxacc[...].astype(BF16)
        if hot_cap:
            last = dgacc[dgacc.shape[0] - 1:, :]
            dg_ref[...] = jnp.where(dg_ref[...] > 0.0, dgacc[0:top_k, :], last)
        else:
            dg_ref[...] = dgacc[0:top_k, :]


def combine(route_t, grad_out, s_out, s_dx, key, gates, o_ret, dx_ret, cap, hot=None):
    tok, d = grad_out.shape
    num_exp = key.shape[0]
    top_k = route_t.shape[0]
    rows_spec = pl.BlockSpec((GROUP, cap, d), lambda i: (i, 0, 0))
    key_spec = pl.BlockSpec((GROUP, tok), lambda i: (i, 0))
    ins = [route_t, grad_out, s_out, s_dx, key, gates, o_ret, dx_ret]
    specs = [whole((top_k, tok)), whole((tok, d)), whole((tok, d)), whole((tok, d)), key_spec, key_spec,
             rows_spec, rows_spec]
    hot_cap = hot_exp = 0
    if hot is not None:
        hot_exp, hot_cap = hot[2].shape[:2]
        ins += list(hot)
        specs += [whole(a.shape) for a in hot]
    return pl.pallas_call(
        functools.partial(combine_kernel, cap=cap, hot_cap=hot_cap, hot_exp=hot_exp),
        grid=(num_exp // GROUP,), in_specs=specs,
        out_specs=[whole((tok, d)), whole((tok, d)), whole((top_k, tok))],
        out_shape=[jax.ShapeDtypeStruct((tok, d), BF16), jax.ShapeDtypeStruct((tok, d), BF16),
                   jax.ShapeDtypeStruct((top_k, tok), F32)],
        scratch_shapes=[pltpu.VMEM((tok, d), F32), pltpu.VMEM((tok, d), F32), pltpu.VMEM((8, tok), F32)],
        cost_estimate=pl.CostEstimate(flops=10 * num_exp * cap * tok * d, bytes_accessed=4 * num_exp * cap * d,
                                      transcendentals=0),
        compiler_params=cparams(), name="combine",
    )(*ins)


def shared_kernel(x_ref, g_ref, wg_ref, wu_ref, wd_ref, o_ref, dx_ref, dwg_ref, dwu_ref, dwd_ref, oacc, dxacc):
    i = pl.program_id(0)
    x = x_ref[...]
    c = g_ref[...]
    wg, wu, wd = wg_ref[...], wu_ref[...], wd_ref[...]
    u = dot_nn(x, wg).astype(BF16).astype(F32)
    v = dot_nn(x, wu).astype(BF16).astype(F32)
    sig = jax.nn.sigmoid(u)
    silu = u * sig
    a = (silu * v).astype(BF16)
    da = dot_nt(c, wd).astype(BF16).astype(F32)
    du = (da * v * sig * (1.0 + u * (1.0 - sig))).astype(BF16)
    dv = (da * silu).astype(BF16)
    o = dot_nn(a, wd)
    dx = dot_nt(du, wg) + dot_nt(dv, wu)

    @pl.when(i == 0)
    def _():
        oacc[...] = o
        dxacc[...] = dx

    @pl.when(i > 0)
    def _():
        oacc[...] += o
        dxacc[...] += dx

    dwd_ref[0] = dot_tn(a, c)
    dwg_ref[0] = dot_tn(x, du)
    dwu_ref[0] = dot_tn(x, dv)

    @pl.when(i == pl.num_programs(0) - 1)
    def _():
        o_ref[...] = oacc[...].astype(BF16)
        dx_ref[...] = dxacc[...].astype(BF16)


def shared_expert(tokens, grad_out, wg, wu, wd):
    tok, d = tokens.shape
    f = wg.shape[1]
    ft = f // 2
    return pl.pallas_call(
        shared_kernel, grid=(f // ft,),
        in_specs=[whole((tok, d)), whole((tok, d)), pl.BlockSpec((d, ft), lambda i: (0, i)),
                  pl.BlockSpec((d, ft), lambda i: (0, i)), pl.BlockSpec((ft, d), lambda i: (i, 0))],
        out_specs=[whole((tok, d)), whole((tok, d)), pl.BlockSpec((1, d, ft), lambda i: (0, 0, i)),
                   pl.BlockSpec((1, d, ft), lambda i: (0, 0, i)), pl.BlockSpec((1, ft, d), lambda i: (0, i, 0))],
        out_shape=[jax.ShapeDtypeStruct((tok, d), BF16), jax.ShapeDtypeStruct((tok, d), BF16),
                   jax.ShapeDtypeStruct((1, d, f), F32), jax.ShapeDtypeStruct((1, d, f), F32),
                   jax.ShapeDtypeStruct((1, f, d), F32)],
        scratch_shapes=[pltpu.VMEM((tok, d), F32), pltpu.VMEM((tok, d), F32)],
        cost_estimate=pl.CostEstimate(flops=18 * tok * d * f, bytes_accessed=18 * d * f, transcendentals=0),
        compiler_params=cparams(), name="shared_expert",
    )(tokens, grad_out, wg, wu, wd)


def device_of(index, n_x, n_c):
    return {"ey": index // (n_x * n_c), "ex": lax.rem(index // n_c, n_x), "ec": lax.rem(index, n_c)}


def flag_kernel(flag_ref, out_ref, send_sem, recv_sem, *, n_dev, n_x, n_c):
    me = lax.axis_index(EP_AXES)
    barrier = pltpu.get_barrier_semaphore()

    def greet(i, carry):
        pl.semaphore_signal(barrier, inc=1, device_id=device_of(lax.rem(me + i, n_dev), n_x, n_c),
                            device_id_type=MESH_ID)
        return carry

    lax.fori_loop(1, n_dev, greet, 0)
    pl.semaphore_wait(barrier, n_dev - 1)

    def copy(i):
        return pltpu.make_async_remote_copy(
            src_ref=flag_ref, dst_ref=out_ref.at[i], send_sem=send_sem.at[i], recv_sem=recv_sem.at[i],
            device_id=device_of(lax.rem(me + i, n_dev), n_x, n_c), device_id_type=MESH_ID)

    def start(i, carry):
        copy(i).start()
        return carry

    def finish(i, carry):
        copy(i).wait()
        return carry

    lax.fori_loop(1, n_dev, start, 0)
    out_ref[0] = flag_ref[...]
    lax.fori_loop(1, n_dev, finish, 0)


def all_flags(flag, mesh_shape):
    n_dev = mesh_shape["ey"] * mesh_shape["ex"] * mesh_shape["ec"]
    out = pl.pallas_call(
        functools.partial(flag_kernel, n_dev=n_dev, n_x=mesh_shape["ex"], n_c=mesh_shape["ec"]),
        out_shape=jax.ShapeDtypeStruct((n_dev,) + flag.shape, flag.dtype),
        in_specs=[pl.BlockSpec(memory_space=pltpu.VMEM)], out_specs=pl.BlockSpec(memory_space=pltpu.VMEM),
        scratch_shapes=[pltpu.SemaphoreType.DMA((n_dev,)), pltpu.SemaphoreType.DMA((n_dev,))],
        compiler_params=pltpu.CompilerParams(collective_id=1, has_side_effects=True), name="flags",
    )(flag)
    return jnp.max(out[:, 0, 1]) > 0.0


def exchange(rows):
    return lax.all_to_all(rows, EP_AXES, 0, 0, tiled=False)


def solution(mesh):
    shape = dict(mesh.shape)
    n_dev = shape["ey"] * shape["ex"] * shape["ec"]
    n_chips = shape["ey"] * shape["ex"]
    n_core = shape["ec"]

    def device_step(tokens, route_idx, gate_vals, w_gate, w_up, w_down, ws_gate, ws_up, ws_down, grad_out):
        tok, top_k = route_idx.shape
        d = tokens.shape[1]
        exp_dev = w_gate.shape[0]
        num_exp = exp_dev * n_dev
        hot_exp = num_exp // n_chips
        mean_cold = -(-((top_k - 1) * tok) // (num_exp - hot_exp))
        cap = -(-mean_cold // 16) * 16
        full_cap = tok // hot_exp
        route_t = route_idx.T
        gate_t = gate_vals.T

        def dev_rows(rows):
            return rows.reshape(n_dev, exp_dev, rows.shape[-2], d)

        def exp_rows(rows):
            return rows.reshape(num_exp, rows.shape[-2], d)

        send_x, key, gates, hkey, hgate, meta = gather_x(route_t, gate_t, tokens, num_exp, hot_exp, True, cap)
        hot_set = meta[0, 0].astype(jnp.int32)
        x_rows = exchange(dev_rows(send_x))
        send_c = gather_cot(key, gates, grad_out, cap)
        c_rows = exchange(dev_rows(send_c))
        overflow = all_flags(meta, shape)

        core = lax.axis_index("ec")
        chip = lax.axis_index(("ey", "ex"))
        is_hot = chip == hot_set
        place = jnp.logical_and(jnp.arange(n_core) == core, is_hot)[:, None, None, None]

        def share_weights(w):
            spread = jnp.where(place, w[None], jnp.zeros((), w.dtype))
            return lax.psum(spread, EP_AXES).reshape((hot_exp,) + w.shape[1:])

        hot_w = [share_weights(w) for w in (w_gate, w_up, w_down)]
        s_out, s_dx, dws_gate, dws_up, dws_down = shared_expert(tokens, grad_out, ws_gate, ws_up, ws_down)
        ho, hdx, *hot_dw = hot_expert(hkey, hgate, tokens, grad_out, *hot_w, full_cap)
        hot_dw = [lax.psum(w, EP_AXES) for w in hot_dw]

        o_rows, dx_rows, *cold_dw = ffn(x_rows, c_rows, w_gate, w_up, w_down, 8)
        o_ret = exchange(o_rows)
        dx_ret = exchange(dx_rows)
        y, dx, dg = combine(route_t, grad_out, s_out, s_dx, key, gates, exp_rows(o_ret), exp_rows(dx_ret), cap,
                            (hkey, hgate, ho, hdx))
        dws = []
        for hot, cold in zip(hot_dw, cold_dw):
            mine = lax.dynamic_slice_in_dim(hot, core * exp_dev, exp_dev, 0)
            dws.append(jnp.where(is_hot, mine, cold))

        def general(_):
            sx, key, gates, *_rest = gather_x(route_t, gate_t, tokens, num_exp, hot_exp, False, full_cap)
            sc = gather_cot(key, gates, grad_out, full_cap)
            xr = exchange(dev_rows(sx))
            cr = exchange(dev_rows(sc))
            orow, dxrow, *dw = ffn(xr, cr, w_gate, w_up, w_down, 4)
            out = combine(route_t, grad_out, s_out, s_dx, key, gates, exp_rows(exchange(orow)),
                          exp_rows(exchange(dxrow)), full_cap)
            return tuple(out) + tuple(dw)

        fast = (y, dx, dg) + tuple(dws)
        y, dx, dg, dw_gate, dw_up, dw_down = lax.cond(overflow, general, lambda outs: outs, fast)
        return y, dx, dg.T, dw_gate, dw_up, dw_down, dws_gate, dws_up, dws_down

    tok_spec = P(ALL_AXES, None)
    exp_spec = P(EP_AXES, None, None)
    rep_spec = P(None, None)
    grad_spec = P(ALL_AXES, None, None)
    return jax.shard_map(
        device_step, mesh=mesh,
        in_specs=(tok_spec, tok_spec, tok_spec, exp_spec, exp_spec, exp_spec, rep_spec, rep_spec, rep_spec, tok_spec),
        out_specs=(tok_spec, tok_spec, tok_spec, grad_spec, grad_spec, grad_spec, grad_spec, grad_spec, grad_spec),
        check_vma=False)
```

```python
import functools

import jax
import jax.numpy as jnp
from jax import lax
from jax.experimental import pallas as pl
from jax.experimental.pallas import tpu as pltpu
from jax.sharding import PartitionSpec as P


EP_AXES = ("ey", "ex", "ec")
ALL_AXES = ("dp", "ey", "ex", "ec")
F32 = jnp.float32
BF16 = jnp.bfloat16
MESH_ID = pl.DeviceIdType.MESH
VMEM_LIMIT = 60 * 1024 * 1024
GROUP = 8


def dot_nn(a, b):
    return lax.dot_general(a, b, (((1,), (0,)), ((), ())), preferred_element_type=F32)


def dot_nt(a, b):
    return lax.dot_general(a, b, (((1,), (1,)), ((), ())), preferred_element_type=F32)


def dot_tn(a, b):
    return lax.dot_general(a, b, (((0,), (0,)), ((), ())), preferred_element_type=F32)


def cparams(**kw):
    return pltpu.CompilerParams(vmem_limit_bytes=VMEM_LIMIT, **kw)


def whole(shape):
    return pl.BlockSpec(shape, lambda *_: (0,) * len(shape))


def forward_rows(x, w_gate, w_up, w_down):
    u = dot_nn(x, w_gate).astype(BF16)
    v = dot_nn(x, w_up).astype(BF16)
    u32 = u.astype(F32)
    a = (u32 * jax.nn.sigmoid(u32) * v.astype(F32)).astype(BF16)
    return u, v, dot_nn(a, w_down).astype(BF16)


def backward_rows(c, u, v, w_gate, w_up, w_down):
    u, v = u.astype(F32), v.astype(F32)
    sig = jax.nn.sigmoid(u)
    silu = u * sig
    a = (silu * v).astype(BF16)
    da = dot_nt(c, w_down).astype(BF16).astype(F32)
    du = (da * v * sig * (1.0 + u * (1.0 - sig))).astype(BF16)
    dv = (da * silu).astype(BF16)
    dx = (dot_nt(du, w_gate) + dot_nt(dv, w_up)).astype(BF16)
    return dx, a, du, dv


def swiglu_rows(x, c, w_gate, w_up, w_down):
    u, v, o = forward_rows(x, w_gate, w_up, w_down)
    return (o,) + backward_rows(c, u, v, w_gate, w_up, w_down)


def routing_tables(route_ref, gate_ref, core_ref, num_exp, hot_exp, n_core, local_hot, cap):
    top_k, tok = route_ref.shape
    route = route_ref[...]
    gate = gate_ref[...]
    exp_id = lax.broadcasted_iota(jnp.int32, (num_exp, tok), 0)
    member = jnp.zeros((num_exp, tok), F32)
    gates = jnp.zeros((num_exp, tok), F32)
    for j in range(top_k):
        hit = exp_id == route[j:j + 1, :]
        member = jnp.where(hit, 1.0, member)
        gates = jnp.where(hit, gate[j:j + 1, :], gates)
    before = (lax.broadcasted_iota(jnp.int32, (tok, tok), 0)
              < lax.broadcasted_iota(jnp.int32, (tok, tok), 1)).astype(F32).astype(BF16)
    rank = dot_nn(member.astype(BF16), before)
    counts = jnp.sum(member, axis=1, keepdims=True)
    if not local_hot:
        return jnp.where(member > 0.0, rank, -1.0), gates, None, None, None
    n_sets = num_exp // hot_exp
    set_of = lax.broadcasted_iota(jnp.int32, (n_sets, num_exp), 1) // hot_exp
    in_set = (set_of == lax.broadcasted_iota(jnp.int32, (n_sets, num_exp), 0)).astype(F32).astype(BF16)
    per_set = dot_nn(in_set, member.astype(BF16))
    full = jnp.min(jnp.where(per_set == 1.0, 1.0, 0.0), axis=1, keepdims=True)
    set_id = lax.broadcasted_iota(jnp.int32, (n_sets, 1), 0).astype(F32)
    hot = jnp.min(jnp.where(full > 0.0, set_id, float(n_sets)), axis=0, keepdims=True)
    n_full = jnp.sum(full, axis=0, keepdims=True)
    exp_col = lax.broadcasted_iota(jnp.int32, (num_exp, 1), 0).astype(F32)
    first = hot * float(hot_exp)
    is_hot = jnp.logical_and(exp_col >= first, exp_col < first + float(hot_exp))
    key = jnp.where(member > 0.0, rank, -1.0)
    hot_keys, hot_gates = [], []
    per_core = hot_exp // n_core
    core = core_ref[0:1, 0:1]
    for h in range(hot_exp):
        plane = core + float(h // per_core)
        plane = jnp.where(plane >= float(n_core), plane - float(n_core), plane)
        pick = exp_col == first + plane * float(per_core) + float(h % per_core)
        hot_keys.append(jnp.sum(jnp.where(pick, key + 1.0, 0.0), axis=0, keepdims=True) - 1.0)
        hot_gates.append(jnp.sum(jnp.where(pick, gates, 0.0), axis=0, keepdims=True))
    key = jnp.where(is_hot, -1.0, key)
    most = jnp.max(jnp.where(is_hot, 0.0, counts), axis=0, keepdims=True)
    bad = jnp.where(jnp.logical_or(most > float(cap), n_full != 1.0), 1.0, 0.0)
    return key, gates, jnp.concatenate(hot_keys, axis=0), jnp.concatenate(hot_gates, axis=0), (hot, bad)


def pick_mask(key_rows, cap):
    tok = key_rows.shape[1]
    rank = lax.broadcasted_iota(jnp.int32, (cap, tok), 0).astype(F32)
    return [key_rows[e:e + 1, :] == rank for e in range(key_rows.shape[0])]


def as_bf16(mask):
    return jnp.where(mask, 1.0, 0.0).astype(BF16)


def gather_x_kernel(route_ref, gate_ref, core_ref, x_ref, send_ref, key_ref, gates_ref, hkey_ref, hgate_ref, meta_ref,
                    *, num_exp, hot_exp, n_core, local_hot, cap):
    i = pl.program_id(0)

    @pl.when(i == 0)
    def _():
        key, gates, hkey, hgate, meta = routing_tables(route_ref, gate_ref, core_ref, num_exp, hot_exp, n_core, local_hot,
                                                       cap)
        key_ref[...] = key
        gates_ref[...] = gates
        if local_hot:
            hkey_ref[...] = hkey
            hgate_ref[...] = hgate
            lane = lax.broadcasted_iota(jnp.int32, (8, 128), 1)
            meta_ref[...] = jnp.where(lane == 0, meta[0], jnp.where(lane == 1, meta[1], 0.0))
        else:
            hkey_ref[...] = jnp.zeros_like(hkey_ref)
            hgate_ref[...] = jnp.zeros_like(hgate_ref)
            meta_ref[...] = jnp.zeros_like(meta_ref)

    keys = key_ref[pl.ds(pl.multiple_of(i * GROUP, GROUP), GROUP), :]
    x = x_ref[...]
    sel = jnp.concatenate([as_bf16(m) for m in pick_mask(keys, cap)], axis=0)
    send_ref[...] = dot_nn(sel, x).astype(BF16).reshape(send_ref.shape)


def gather_x(route_t, gate_t, core, tokens, num_exp, hot_exp, n_core, local_hot, cap):
    tok, d = tokens.shape
    top_k = route_t.shape[0]
    return pl.pallas_call(
        functools.partial(gather_x_kernel, num_exp=num_exp, hot_exp=hot_exp, n_core=n_core, local_hot=local_hot,
                          cap=cap),
        grid=(num_exp // GROUP,),
        in_specs=[whole((top_k, tok)), whole((top_k, tok)), whole(core.shape), whole((tok, d))],
        out_specs=[pl.BlockSpec((GROUP, cap, d), lambda i: (i, 0, 0)), whole((num_exp, tok)), whole((num_exp, tok)),
                   whole((hot_exp, tok)), whole((hot_exp, tok)), whole((8, 128))],
        out_shape=[jax.ShapeDtypeStruct((num_exp, cap, d), BF16), jax.ShapeDtypeStruct((num_exp, tok), F32),
                   jax.ShapeDtypeStruct((num_exp, tok), F32), jax.ShapeDtypeStruct((hot_exp, tok), F32),
                   jax.ShapeDtypeStruct((hot_exp, tok), F32), jax.ShapeDtypeStruct((8, 128), F32)],
        cost_estimate=pl.CostEstimate(flops=2 * num_exp * cap * tok * d, bytes_accessed=2 * num_exp * cap * d,
                                      transcendentals=0),
        compiler_params=cparams(), name="gather_x",
    )(route_t, gate_t, core, tokens)


def cot_rows(masks, gate_rows, g):
    sel = jnp.concatenate([as_bf16(m) for m in masks], axis=0)
    gate_col = jnp.concatenate(
        [jnp.sum(jnp.where(m, gate_rows[e:e + 1, :], 0.0), axis=1, keepdims=True) for e, m in enumerate(masks)], axis=0)
    return sel, (gate_col * dot_nn(sel, g)).astype(BF16)


def gather_cot_kernel(key_ref, gates_ref, g_ref, send_ref, *, cap):
    masks = pick_mask(key_ref[...], cap)
    send_ref[...] = cot_rows(masks, gates_ref[...], g_ref[...])[1].reshape(send_ref.shape)


def gather_cot(key, gates, grad_out, cap):
    num_exp, tok = key.shape
    d = grad_out.shape[1]
    return pl.pallas_call(
        functools.partial(gather_cot_kernel, cap=cap),
        grid=(num_exp // GROUP,),
        in_specs=[pl.BlockSpec((GROUP, tok), lambda i: (i, 0)), pl.BlockSpec((GROUP, tok), lambda i: (i, 0)),
                  whole((tok, d))],
        out_specs=pl.BlockSpec((GROUP, cap, d), lambda i: (i, 0, 0)),
        out_shape=jax.ShapeDtypeStruct((num_exp, cap, d), BF16),
        cost_estimate=pl.CostEstimate(flops=2 * num_exp * cap * tok * d, bytes_accessed=2 * num_exp * cap * d,
                                      transcendentals=0),
        compiler_params=cparams(), name="gather_cot",
    )(key, gates, grad_out)


def hot_gather_kernel(hkey_ref, hgate_ref, x_ref, g_ref, own_ref, other_ref, *, cap):
    hot_exp = hkey_ref.shape[0]
    half = hot_exp // 2
    masks = pick_mask(hkey_ref[...], cap)
    sel, c = cot_rows(masks, hgate_ref[...], g_ref[...])
    x = dot_nn(sel, x_ref[...]).astype(BF16)
    shape = own_ref.shape[1:]
    own_ref[0] = x[:half * cap].reshape(shape)
    own_ref[1] = c[:half * cap].reshape(shape)
    other_ref[0] = x[half * cap:].reshape(shape)
    other_ref[1] = c[half * cap:].reshape(shape)


def hot_gather(hkey, hgate, tokens, grad_out, cap):
    hot_exp = hkey.shape[0]
    tok, d = tokens.shape
    rows = jax.ShapeDtypeStruct((2, hot_exp // 2, cap, d), BF16)
    return pl.pallas_call(
        functools.partial(hot_gather_kernel, cap=cap), out_shape=[rows, rows],
        cost_estimate=pl.CostEstimate(flops=4 * hot_exp * cap * tok * d, bytes_accessed=4 * hot_exp * cap * d,
                                      transcendentals=0),
        compiler_params=cparams(), name="hot_gather",
    )(hkey, hgate, tokens, grad_out)


def hot_kernel(own_ref, their_ref, wg_ref, wu_ref, wd_ref, flag_ref, own_out, their_out, dwg_ref, dwu_ref, dwd_ref):
    f, d = wd_ref.shape[1:]
    cap = own_ref.shape[2]
    x = jnp.concatenate([own_ref[0, 0], their_ref[0, 0]], axis=0)
    c = jnp.concatenate([own_ref[1, 0], their_ref[1, 0]], axis=0)
    o, dx, a, du, dv = swiglu_rows(x, c, wg_ref[0], wu_ref[0], wd_ref[0])
    own_out[0, 0] = o[:cap]
    own_out[1, 0] = dx[:cap]
    their_out[0, 0] = o[cap:]
    their_out[1, 0] = dx[cap:]
    dwd_ref[0, :f, :] = dot_tn(a, c)
    dwd_ref[0, f:, :] = jnp.broadcast_to(flag_ref[0:1, 1:2], (8, d))
    dwg_ref[0] = dot_tn(x, du)
    dwu_ref[0] = dot_tn(x, dv)


def hot_expert(own, theirs, wg, wu, wd, flag):
    n_exp, cap = own.shape[1:3]
    d, f = wg.shape[1:]
    row_spec = pl.BlockSpec((2, 1, cap, d), lambda e: (0, e, 0, 0))
    up_spec = pl.BlockSpec((1, d, f), lambda e: (e, 0, 0))
    down_spec = pl.BlockSpec((1, f, d), lambda e: (e, 0, 0))
    return pl.pallas_call(
        hot_kernel, grid=(n_exp,),
        in_specs=[row_spec, row_spec, up_spec, up_spec, down_spec, whole(flag.shape)],
        out_specs=[row_spec, row_spec, up_spec, up_spec, pl.BlockSpec((1, f + 8, d), lambda e: (e, 0, 0))],
        out_shape=[jax.ShapeDtypeStruct(own.shape, BF16), jax.ShapeDtypeStruct(own.shape, BF16),
                   jax.ShapeDtypeStruct(wg.shape, F32), jax.ShapeDtypeStruct(wu.shape, F32),
                   jax.ShapeDtypeStruct((n_exp, f + 8, d), F32)],
        cost_estimate=pl.CostEstimate(flops=36 * n_exp * cap * d * f, bytes_accessed=20 * n_exp * d * f,
                                      transcendentals=0),
        compiler_params=cparams(), name="hot_expert",
    )(own, theirs, wg, wu, wd, flag)


def rows_of(ref):
    return ref[...].reshape(ref.shape[0] * ref.shape[2], ref.shape[3])


def cold_forward_kernel(x_ref, wg_ref, wu_ref, wd_ref, o_ref, u_ref, v_ref):
    u, v, o = forward_rows(rows_of(x_ref), wg_ref[0], wu_ref[0], wd_ref[0])
    o_ref[...] = o.reshape(o_ref.shape)
    u_ref[...] = u.reshape(u_ref.shape)
    v_ref[...] = v.reshape(v_ref.shape)


def cold_backward_kernel(x_ref, c_ref, u_ref, v_ref, wg_ref, wu_ref, wd_ref, dx_ref, dwg_ref, dwu_ref, dwd_ref):
    x = rows_of(x_ref)
    c = rows_of(c_ref)
    dx, a, du, dv = backward_rows(c, rows_of(u_ref), rows_of(v_ref), wg_ref[0], wu_ref[0], wd_ref[0])
    dx_ref[...] = dx.reshape(dx_ref.shape)
    first = pl.program_id(1) == 0

    @pl.when(first)
    def _():
        dwd_ref[0] = dot_tn(a, c)
        dwg_ref[0] = dot_tn(x, du)
        dwu_ref[0] = dot_tn(x, dv)

    @pl.when(jnp.logical_not(first))
    def _():
        dwd_ref[0] += dot_tn(a, c)
        dwg_ref[0] += dot_tn(x, du)
        dwu_ref[0] += dot_tn(x, dv)


def cold_specs(cap, d, f, src_tile):
    rows = pl.BlockSpec((src_tile, 1, cap, d), lambda e, s: (s, e, 0, 0))
    acts = pl.BlockSpec((src_tile, 1, cap, f), lambda e, s: (s, e, 0, 0))
    up = pl.BlockSpec((1, d, f), lambda e, s: (e, 0, 0))
    down = pl.BlockSpec((1, f, d), lambda e, s: (e, 0, 0))
    return rows, acts, up, down


def cold_forward(x_rows, wg, wu, wd, src_tile):
    n_src, exp_dev, cap, d = x_rows.shape
    f = wg.shape[2]
    rows, acts, up, down = cold_specs(cap, d, f, src_tile)
    n_rows = n_src * exp_dev * cap
    act_shape = jax.ShapeDtypeStruct((n_src, exp_dev, cap, f), BF16)
    return pl.pallas_call(
        cold_forward_kernel, grid=(exp_dev, n_src // src_tile),
        in_specs=[rows, up, up, down], out_specs=[rows, acts, acts],
        out_shape=[jax.ShapeDtypeStruct(x_rows.shape, BF16), act_shape, act_shape],
        cost_estimate=pl.CostEstimate(flops=6 * n_rows * d * f, bytes_accessed=7 * n_rows * d, transcendentals=0),
        compiler_params=cparams(), name="cold_forward",
    )(x_rows, wg, wu, wd)


def cold_backward(x_rows, c_rows, u_rows, v_rows, wg, wu, wd, src_tile):
    n_src, exp_dev, cap, d = x_rows.shape
    f = wg.shape[2]
    rows, acts, up, down = cold_specs(cap, d, f, src_tile)
    n_rows = n_src * exp_dev * cap
    return pl.pallas_call(
        cold_backward_kernel, grid=(exp_dev, n_src // src_tile),
        in_specs=[rows, rows, acts, acts, up, up, down], out_specs=[rows, up, up, down],
        out_shape=[jax.ShapeDtypeStruct(x_rows.shape, BF16), jax.ShapeDtypeStruct(wg.shape, F32),
                   jax.ShapeDtypeStruct(wu.shape, F32), jax.ShapeDtypeStruct(wd.shape, F32)],
        cost_estimate=pl.CostEstimate(flops=12 * n_rows * d * f, bytes_accessed=9 * n_rows * d, transcendentals=0),
        compiler_params=cparams(), name="cold_backward",
    )(x_rows, c_rows, u_rows, v_rows, wg, wu, wd)


def split3(g):
    hi = g.astype(BF16)
    rest = g - hi.astype(F32)
    mid = rest.astype(BF16)
    lo = (rest - mid.astype(F32)).astype(BF16)
    return hi.astype(F32), mid.astype(F32), lo.astype(F32)


def combine_y_rows(key_rows, gate_rows, o, g, cap):
    masks = pick_mask(key_rows, cap)
    y = None
    for part in split3(gate_rows):
        wt = jnp.concatenate([jnp.where(m, part[e:e + 1, :], 0.0).astype(BF16) for e, m in enumerate(masks)], axis=0)
        term = dot_tn(wt, o)
        y = term if y is None else y + term
    inner = dot_nt(o, g)
    dg = [jnp.sum(jnp.where(m, inner[e * cap:(e + 1) * cap, :], 0.0), axis=0, keepdims=True)
          for e, m in enumerate(masks)]
    return y, jnp.concatenate(dg, axis=0)


def combine_dx_rows(key_rows, dx, cap):
    return dot_tn(jnp.concatenate([as_bf16(m) for m in pick_mask(key_rows, cap)], axis=0), dx)


def combine_y_kernel(*refs, cap, hot_cap, hot_exp):
    if hot_cap:
        (route_ref, g_ref, s_ref, key_ref, gates_ref, o_ref, hkey_ref, hgate_ref, own_ref, other_ref,
         y_ref, dg_ref, yacc, dgacc) = refs
    else:
        route_ref, g_ref, s_ref, key_ref, gates_ref, o_ref, y_ref, dg_ref, yacc, dgacc = refs
    i = pl.program_id(0)
    g = g_ref[...]
    d = g.shape[1]

    @pl.when(i == 0)
    def _():
        yacc[...] = s_ref[...].astype(F32)
        dgacc[...] = jnp.zeros_like(dgacc)
        if hot_cap:
            half = hot_exp * hot_cap // 2
            ho = jnp.concatenate([own_ref[0].reshape(half, d), other_ref[0].reshape(half, d)], axis=0)
            y, dg = combine_y_rows(hkey_ref[...], hgate_ref[...], ho, g, hot_cap)
            yacc[...] += y
            mine = hkey_ref[...] >= 0.0
            dgacc[dgacc.shape[0] - 1:, :] = jnp.sum(jnp.where(mine, dg, 0.0), axis=0, keepdims=True)

    y, dg = combine_y_rows(key_ref[...], gates_ref[...], o_ref[...].reshape(GROUP * cap, d), g, cap)
    yacc[...] += y
    route = route_ref[...]
    top_k = route.shape[0]
    held = key_ref[...] >= 0.0
    for j in range(top_k):
        exp_id = lax.broadcasted_iota(jnp.int32, dg.shape, 0) + i * GROUP
        hit = jnp.logical_and(exp_id == route[j:j + 1, :], held)
        dgacc[j:j + 1, :] += jnp.sum(jnp.where(hit, dg, 0.0), axis=0, keepdims=True)
        if hot_cap:
            seen = jnp.sum(jnp.where(hit, 1.0, 0.0), axis=0, keepdims=True)
            dg_ref[j:j + 1, :] = jnp.where(i == 0, seen, dg_ref[j:j + 1, :] + seen)

    @pl.when(i == pl.num_programs(0) - 1)
    def _():
        y_ref[...] = yacc[...].astype(BF16)
        if hot_cap:
            last = dgacc[dgacc.shape[0] - 1:, :]
            dg_ref[...] = jnp.where(dg_ref[...] > 0.0, dgacc[0:top_k, :], last)
        else:
            dg_ref[...] = dgacc[0:top_k, :]


def combine_y(route_t, grad_out, s_out, key, gates, o_ret, cap, hot=None):
    tok, d = grad_out.shape
    num_exp = key.shape[0]
    top_k = route_t.shape[0]
    key_spec = pl.BlockSpec((GROUP, tok), lambda i: (i, 0))
    ins = [route_t, grad_out, s_out, key, gates, o_ret]
    specs = [whole((top_k, tok)), whole((tok, d)), whole((tok, d)), key_spec, key_spec,
             pl.BlockSpec((GROUP, cap, d), lambda i: (i, 0, 0))]
    hot_cap = hot_exp = 0
    if hot is not None:
        hot_exp, hot_cap = hot[0].shape[0], hot[2].shape[2]
        ins += list(hot)
        specs += [whole(a.shape) for a in hot]
    return pl.pallas_call(
        functools.partial(combine_y_kernel, cap=cap, hot_cap=hot_cap, hot_exp=hot_exp),
        grid=(num_exp // GROUP,), in_specs=specs, out_specs=[whole((tok, d)), whole((top_k, tok))],
        out_shape=[jax.ShapeDtypeStruct((tok, d), BF16), jax.ShapeDtypeStruct((top_k, tok), F32)],
        scratch_shapes=[pltpu.VMEM((tok, d), F32), pltpu.VMEM((8, tok), F32)],
        cost_estimate=pl.CostEstimate(flops=8 * num_exp * cap * tok * d, bytes_accessed=2 * num_exp * cap * d,
                                      transcendentals=0),
        compiler_params=cparams(), name="combine_y",
    )(*ins)


def combine_dx_kernel(*refs, cap, hot_cap, hot_exp):
    if hot_cap:
        s_ref, key_ref, dx_ref, hkey_ref, own_ref, other_ref, out_ref, acc = refs
    else:
        s_ref, key_ref, dx_ref, out_ref, acc = refs
    i = pl.program_id(0)
    d = out_ref.shape[1]

    @pl.when(i == 0)
    def _():
        acc[...] = s_ref[...].astype(F32)
        if hot_cap:
            half = hot_exp * hot_cap // 2
            hdx = jnp.concatenate([own_ref[1].reshape(half, d), other_ref[1].reshape(half, d)], axis=0)
            acc[...] += combine_dx_rows(hkey_ref[...], hdx, hot_cap)

    acc[...] += combine_dx_rows(key_ref[...], dx_ref[...].reshape(GROUP * cap, d), cap)

    @pl.when(i == pl.num_programs(0) - 1)
    def _():
        out_ref[...] = acc[...].astype(BF16)


def combine_dx(s_dx, key, dx_ret, cap, hot=None):
    tok, d = s_dx.shape
    num_exp = key.shape[0]
    ins = [s_dx, key, dx_ret]
    specs = [whole((tok, d)), pl.BlockSpec((GROUP, tok), lambda i: (i, 0)),
             pl.BlockSpec((GROUP, cap, d), lambda i: (i, 0, 0))]
    hot_cap = hot_exp = 0
    if hot is not None:
        hot_exp, hot_cap = hot[0].shape[0], hot[1].shape[2]
        ins += list(hot)
        specs += [whole(a.shape) for a in hot]
    return pl.pallas_call(
        functools.partial(combine_dx_kernel, cap=cap, hot_cap=hot_cap, hot_exp=hot_exp),
        grid=(num_exp // GROUP,), in_specs=specs, out_specs=whole((tok, d)),
        out_shape=jax.ShapeDtypeStruct((tok, d), BF16), scratch_shapes=[pltpu.VMEM((tok, d), F32)],
        cost_estimate=pl.CostEstimate(flops=2 * num_exp * cap * tok * d, bytes_accessed=2 * num_exp * cap * d,
                                      transcendentals=0),
        compiler_params=cparams(), name="combine_dx",
    )(*ins)


def shared_kernel(x_ref, g_ref, wg_ref, wu_ref, wd_ref, o_ref, dx_ref, dwg_ref, dwu_ref, dwd_ref, oacc, dxacc):
    i = pl.program_id(0)
    x = x_ref[...]
    c = g_ref[...]
    wg, wu, wd = wg_ref[...], wu_ref[...], wd_ref[...]
    u = dot_nn(x, wg).astype(BF16).astype(F32)
    v = dot_nn(x, wu).astype(BF16).astype(F32)
    sig = jax.nn.sigmoid(u)
    silu = u * sig
    a = (silu * v).astype(BF16)
    da = dot_nt(c, wd).astype(BF16).astype(F32)
    du = (da * v * sig * (1.0 + u * (1.0 - sig))).astype(BF16)
    dv = (da * silu).astype(BF16)
    o = dot_nn(a, wd)
    dx = dot_nt(du, wg) + dot_nt(dv, wu)

    @pl.when(i == 0)
    def _():
        oacc[...] = o
        dxacc[...] = dx

    @pl.when(i > 0)
    def _():
        oacc[...] += o
        dxacc[...] += dx

    dwd_ref[0] = dot_tn(a, c)
    dwg_ref[0] = dot_tn(x, du)
    dwu_ref[0] = dot_tn(x, dv)

    @pl.when(i == pl.num_programs(0) - 1)
    def _():
        o_ref[...] = oacc[...].astype(BF16)
        dx_ref[...] = dxacc[...].astype(BF16)


def shared_expert(tokens, grad_out, wg, wu, wd):
    tok, d = tokens.shape
    f = wg.shape[1]
    ft = f // 2
    return pl.pallas_call(
        shared_kernel, grid=(f // ft,),
        in_specs=[whole((tok, d)), whole((tok, d)), pl.BlockSpec((d, ft), lambda i: (0, i)),
                  pl.BlockSpec((d, ft), lambda i: (0, i)), pl.BlockSpec((ft, d), lambda i: (i, 0))],
        out_specs=[whole((tok, d)), whole((tok, d)), pl.BlockSpec((1, d, ft), lambda i: (0, 0, i)),
                   pl.BlockSpec((1, d, ft), lambda i: (0, 0, i)), pl.BlockSpec((1, ft, d), lambda i: (0, i, 0))],
        out_shape=[jax.ShapeDtypeStruct((tok, d), BF16), jax.ShapeDtypeStruct((tok, d), BF16),
                   jax.ShapeDtypeStruct((1, d, f), F32), jax.ShapeDtypeStruct((1, d, f), F32),
                   jax.ShapeDtypeStruct((1, f, d), F32)],
        scratch_shapes=[pltpu.VMEM((tok, d), F32), pltpu.VMEM((tok, d), F32)],
        cost_estimate=pl.CostEstimate(flops=18 * tok * d * f, bytes_accessed=18 * d * f, transcendentals=0),
        compiler_params=cparams(), name="shared_expert",
    )(tokens, grad_out, wg, wu, wd)


def share_kernel(hot_ref, wg_ref, wu_ref, wd_ref, og_ref, ou_ref, od_ref, *scratch, n_x, n_y, parts):
    n_part = len(parts)
    landed, picked, fine = scratch[:n_part], scratch[n_part:2 * n_part], scratch[2 * n_part:3 * n_part]
    send_sem, recv_sem = scratch[3 * n_part:]
    x, y = lax.axis_index("ex"), lax.axis_index("ey")
    size = {"ex": n_x, "ey": n_y}
    mine = {"ex": x, "ey": y}
    hot = {"ey": hot_ref[0], "ex": hot_ref[1]}
    ins = (wg_ref, wu_ref, wd_ref)
    outs = (og_ref, ou_ref, od_ref)

    barrier = pltpu.get_barrier_semaphore()
    for axis in ("ex", "ey"):
        for step in range(1, size[axis]):
            pl.semaphore_signal(barrier, inc=1, device_id={axis: lax.rem(mine[axis] + step, size[axis])},
                                device_id_type=MESH_ID)
    pl.semaphore_wait(barrier, n_x + n_y - 2)

    def send(stage, part, axis, step, src, dst):
        copy = pltpu.make_async_remote_copy(
            src_ref=src, dst_ref=dst, send_sem=send_sem.at[stage, part, step - 1],
            recv_sem=recv_sem.at[stage, part, step - 1],
            device_id={axis: lax.rem(mine[axis] + step, size[axis])}, device_id_type=MESH_ID)
        copy.start()
        return copy

    def window(start, count):
        return pl.ds(pl.multiple_of(start, 16), count)

    copies = []
    for p, (array, first, second, base, rows) in enumerate(parts):
        block = rows * size[second]
        for step in range(1, size[first]):
            to = lax.rem(mine[first] + step, size[first])
            copies.append(send(0, p, first, step, ins[array].at[window(base + to * block, block)],
                               landed[p].at[mine[first]]))
        landed[p][mine[first]] = ins[array][window(base + mine[first] * block, block), :]
    for copy in copies:
        copy.wait()

    copies = []
    for p, (array, first, second, base, rows) in enumerate(parts):
        picked[p][...] = landed[p][hot[first]]
        for step in range(1, size[second]):
            to = lax.rem(mine[second] + step, size[second])
            copies.append(send(1, p, second, step, picked[p].at[window(to * rows, rows)], fine[p].at[mine[second]]))
        fine[p][mine[second]] = picked[p][window(mine[second] * rows, rows), :]
    for copy in copies:
        copy.wait()

    copies = []
    for p, (array, first, second, base, rows) in enumerate(parts):
        at = base + (mine[first] * size[second] + mine[second]) * rows
        outs[array][window(at, rows), :] = fine[p][hot[second]]
        for step in range(1, size[second]):
            copies.append(send(2, p, second, step, outs[array].at[window(at, rows)], outs[array].at[window(at, rows)]))
    for copy in copies:
        copy.wait()

    copies = []
    for p, (array, first, second, base, rows) in enumerate(parts):
        block = rows * size[second]
        at = base + mine[first] * block
        for step in range(1, size[first]):
            copies.append(send(3, p, first, step, outs[array].at[window(at, block)], outs[array].at[window(at, block)]))
    for copy in copies:
        copy.wait()


def share_weights(hot_yx, weights, mesh_shape):
    n_x, n_y = mesh_shape["ex"], mesh_shape["ey"]
    n_chips = n_x * n_y
    flat = [w.reshape(-1, w.shape[2]) for w in weights]
    total = [w.shape[0] // n_chips for w in flat]
    low = total[2] // 3
    parts = ((0, "ex", "ey", 0, total[0]), (1, "ey", "ex", 0, total[1]),
             (2, "ex", "ey", 0, low), (2, "ey", "ex", low * n_chips, total[2] - low))
    size = {"ex": n_x, "ey": n_y}
    landed, picked, fine = [], [], []
    for array, first, second, _, rows in parts:
        cols = flat[array].shape[1]
        landed.append(pltpu.VMEM((size[first], rows * size[second], cols), BF16))
        picked.append(pltpu.VMEM((rows * size[second], cols), BF16))
        fine.append(pltpu.VMEM((size[second], rows, cols), BF16))
    sems = pltpu.SemaphoreType.DMA((4, len(parts), max(n_x, n_y) - 1))
    vmem = pl.BlockSpec(memory_space=pltpu.VMEM)
    out = pl.pallas_call(
        functools.partial(share_kernel, n_x=n_x, n_y=n_y, parts=parts),
        out_shape=[jax.ShapeDtypeStruct(w.shape, w.dtype) for w in flat],
        in_specs=[pl.BlockSpec(memory_space=pltpu.SMEM), vmem, vmem, vmem], out_specs=[vmem] * 3,
        scratch_shapes=[*landed, *picked, *fine, sems, sems],
        compiler_params=pltpu.CompilerParams(collective_id=1, has_side_effects=True, vmem_limit_bytes=32 * 1024 * 1024),
        cost_estimate=pl.CostEstimate(flops=30_000_000_000, bytes_accessed=0, transcendentals=0), name="share_weights",
    )(hot_yx, *flat)
    return [o.reshape(w.shape) for o, w in zip(out, weights)]


def exchange(rows):
    return lax.all_to_all(rows, EP_AXES, 0, 0, tiled=False)


def solution(mesh):
    shape = dict(mesh.shape)
    n_dev = shape["ey"] * shape["ex"] * shape["ec"]
    n_chips = shape["ey"] * shape["ex"]
    n_core = shape["ec"]

    def layer(tokens, route_idx, gate_vals, w_gate, w_up, w_down, ws_gate, ws_up, ws_down, grad_out):
        tok, top_k = route_idx.shape
        d = tokens.shape[1]
        exp_dev = w_gate.shape[0]
        num_exp = exp_dev * n_dev
        hot_exp = num_exp // n_chips
        mean_cold = -(-((top_k - 1) * tok) // (num_exp - hot_exp))
        cap = -(-mean_cold // 16) * 16
        full_cap = tok // hot_exp
        route_t = route_idx.T
        gate_t = gate_vals.T

        def dev_rows(rows):
            return rows.reshape(n_dev, exp_dev, rows.shape[-2], d)

        def exp_rows(rows):
            return rows.reshape(num_exp, rows.shape[-2], d)

        core = lax.axis_index("ec")
        chip = lax.axis_index(("ey", "ex"))
        core_arr = jnp.full((8, 128), core.astype(F32))
        partner = [(c, (c + 1) % n_core) for c in range(n_core)]

        send_x, key, gates, hkey, hgate, meta = gather_x(route_t, gate_t, core_arr, tokens, num_exp, hot_exp, n_core,
                                                         True, cap)
        hot_chip = meta[0, 0].astype(jnp.int32)
        is_hot = chip == hot_chip
        x_rows = exchange(dev_rows(send_x))
        hot_chip = jnp.minimum(hot_chip, n_chips - 1)
        hot_yx = jnp.stack([hot_chip // shape["ex"], hot_chip % shape["ex"]])
        send_c = gather_cot(key, gates, grad_out, cap)
        own, other = hot_gather(hkey, hgate, tokens, grad_out, full_cap)
        hot_yx, send_c, other = lax.optimization_barrier((hot_yx, send_c, other))
        hot_w = share_weights(hot_yx, (w_gate, w_up, w_down), shape)
        theirs = lax.ppermute(other, "ec", partner)
        flag = jnp.maximum(meta, lax.ppermute(meta, "ec", partner))
        send_c, theirs, hot_w = lax.optimization_barrier((send_c, theirs, hot_w))
        c_rows = exchange(dev_rows(send_c))
        s_out, s_dx, dws_gate, dws_up, dws_down = shared_expert(tokens, grad_out, ws_gate, ws_up, ws_down)

        own_out, their_out, *hot_dw = hot_expert(own, theirs, *hot_w, flag)
        x_rows, their_out = lax.optimization_barrier((x_rows, their_out))
        other_out = lax.ppermute(their_out, "ec", partner)
        hot_dw = list(lax.psum(tuple(hot_dw), ("ey", "ex")))
        f = w_down.shape[1]
        overflow = hot_dw[2][0, f, 0] > 0.0
        hot_dw[2] = hot_dw[2][:, :f]

        o_rows, u_rows, v_rows = cold_forward(x_rows, w_gate, w_up, w_down, 8)
        o_rows, c_rows = lax.optimization_barrier((o_rows, c_rows))
        o_ret = exchange(o_rows)
        dx_rows, *cold_dw = cold_backward(x_rows, c_rows, u_rows, v_rows, w_gate, w_up, w_down, 8)
        dx_ret = exchange(dx_rows)
        y, dg = combine_y(route_t, grad_out, s_out, key, gates, exp_rows(o_ret), cap,
                          (hkey, hgate, own_out, other_out))
        dx = combine_dx(s_dx, key, exp_rows(dx_ret), cap, (hkey, own_out, other_out))
        dws = [jnp.where(is_hot, hot, cold) for hot, cold in zip(hot_dw, cold_dw)]

        def general(_):
            sx, key, gates, *_rest = gather_x(route_t, gate_t, core_arr, tokens, num_exp, hot_exp, n_core, False,
                                              full_cap)
            sc = gather_cot(key, gates, grad_out, full_cap)
            xr = exchange(dev_rows(sx))
            cr = exchange(dev_rows(sc))
            orow, ur, vr = cold_forward(xr, w_gate, w_up, w_down, 4)
            dxrow, *dw = cold_backward(xr, cr, ur, vr, w_gate, w_up, w_down, 4)
            y, dg = combine_y(route_t, grad_out, s_out, key, gates, exp_rows(exchange(orow)), full_cap)
            dx = combine_dx(s_dx, key, exp_rows(exchange(dxrow)), full_cap)
            return (y, dx, dg) + tuple(dw)

        fast = (y, dx, dg) + tuple(dws)
        y, dx, dg, dw_gate, dw_up, dw_down = lax.cond(overflow, general, lambda outs: outs, fast)
        return y, dx, dg.T, dw_gate, dw_up, dw_down, dws_gate, dws_up, dws_down

    tok_spec = P(ALL_AXES, None)
    exp_spec = P(EP_AXES, None, None)
    rep_spec = P(None, None)
    grad_spec = P(ALL_AXES, None, None)
    return jax.shard_map(
        layer, mesh=mesh,
        in_specs=(tok_spec, tok_spec, tok_spec, exp_spec, exp_spec, exp_spec, rep_spec, rep_spec, rep_spec, tok_spec),
        out_specs=(tok_spec, tok_spec, tok_spec, grad_spec, grad_spec, grad_spec, grad_spec, grad_spec, grad_spec),
        check_vma=False)
```
